256 devices in a mesh: rows: 2 (over core), cols: 4 (over y), slabs: 8 (over z), site: 4 (over x).
Axes of the slice: x: 4, y: 4, z: 8, core: 2. Of those that a mesh axis runs over, the one named last changes fastest.
Arguments:
- field_values: float32 [768, 32, 64, 128], P(('site', 'rows'), 'cols', 'slabs'), parts along dimension 0, may hold values from 0.5 to 2
- crowding: float32 [768, 32, 64, 128], P(('site', 'rows'), 'cols', 'slabs'), parts along dimension 0, may hold values from 0.5 to 2
Outputs:
- standardized: float32 [768, 32, 64, 128], P(('site', 'rows'), 'cols', 'slabs'), parts along dimension 0
- field_values_end: float32 [768, 32, 64, 128], P(('site', 'rows'), 'cols', 'slabs'), parts along dimension 0
The draws below stay inside these ranges and needn't reach their ends.
There are 4 independent parts, one for each index of `site`. The reference program is written for one: setup_inputs(seed, part) draws one part's arguments, and reference() takes and returns one part's arrays. A program takes and returns all parts, laid end to end along the dimension named above; each array names one. Nothing has to cross between parts.
All inputs are finite; a program needn't handle non-finite values.
Results may differ from the reference program's by a relative error of at most 0.000036.
Values sent between devices are 32-bit elements; how exact they have to be, the bound alone decides.
A program may use at most 64 MiB of HBM per device.

```python
import jax
import jax.numpy as jnp
from jax import lax

GRID_Y = 192
GRID_X = 32
GRID_Z = 64
LEVELS = 128
STEPS = 6


def levels(own_key, extent, cuts, low, top_value):
    gain, own = 1.0, jax.random.fold_in(own_key, 6)
    for axis_at, shards_of in cuts:
        draws = jnp.exp(jax.random.uniform(jax.random.fold_in(own, axis_at), (shards_of,), jnp.float32, low / len(cuts), top_value / len(cuts)))
        gain = gain * jnp.repeat(draws, extent[axis_at] // shards_of).reshape([-1 if axis == axis_at else 1 for axis in range(len(extent))])
    return gain


def setup_inputs(seed: int = 0, part: int = 0) -> dict:
    keys = jax.random.split(jax.random.key(seed), 3)
    part_splits = jax.random.split(jax.random.fold_in(keys[2], part), 3)
    field_values = jnp.clip(0.5 + 1.5 * jax.random.uniform(part_splits[0], (GRID_Y, GRID_X, GRID_Z, LEVELS), jnp.float32) ** levels(part_splits[0], (GRID_Y, GRID_X, GRID_Z, LEVELS), ((0, 2), (1, 4), (2, 8)), -0.2, 0.2), 0.5, 2.0)
    crowding = jnp.clip(0.5 + 1.5 * jax.random.uniform(part_splits[1], (GRID_Y, GRID_X, GRID_Z, LEVELS), jnp.float32) ** levels(part_splits[1], (GRID_Y, GRID_X, GRID_Z, LEVELS), ((0, 2), (1, 4), (2, 8)), -0.2, 0.2), 0.5, 2.0)
    return {"field_values": field_values, "crowding": crowding}


def inner_cells(values, dims):
    for dim in dims:
        values = lax.slice_in_dim(values, 1, values.shape[dim] - 1, axis=dim)
    return values

def side_cells(values, dim, start, dims):
    others = [other for other in dims if other != dim]
    values = inner_cells(values, others)
    return lax.slice_in_dim(values, start, start + values.shape[dim] - 2, axis=dim)

def advance(padded, crowding):
    middle = inner_cells(padded, (0, 1, 2))
    lower = [side_cells(padded, dim, 0, (0, 1, 2)) for dim in (0, 1, 2)]
    upper = [side_cells(padded, dim, 2, (0, 1, 2)) for dim in (0, 1, 2)]
    spread = lower[0] + upper[0] + lower[1] + upper[1] + lower[2] + upper[2] - 6.0 * middle
    return middle + 0.1 * spread + 0.2 * middle * (1.0 - middle * crowding)

def reference(field_values, crowding):
    for step in range(STEPS):
        field_values = advance(jnp.pad(field_values, ((1, 1), (1, 1), (1, 1), (0, 0)), mode='wrap'), crowding)
    line_mean = lax.optimization_barrier(jnp.mean(field_values, axis=0, keepdims=True))
    centred = field_values - line_mean
    line_variance = lax.optimization_barrier(jnp.mean(centred * centred, axis=0, keepdims=True))
    standardized = centred * lax.rsqrt(line_variance + 0.0001)
    return (standardized, field_values)
```

```python
import functools

import jax
import jax.numpy as jnp
from jax import lax
from jax.experimental import pallas as pl
from jax.experimental.pallas import tpu as pltpu
from jax.sharding import PartitionSpec as P

STEPS = 6
CHUNKS = 6
MESH = pl.DeviceIdType.MESH
Z = 8


def evolve(sizes, f_hbm, c_hbm, end_ref, mean_ref, scale_ref, field, crowd, shift, first, second,
           mine, theirs, load_sem, crowd_sem, send_sem, recv_sem, row_send, row_recv, stat_send, stat_recv):
    rows, cols, slabs = sizes
    height, width, depth, _ = f_hbm.shape
    part = height // CHUNKS
    me_row, me_col, me_slab = (lax.axis_index(axis) for axis in ("rows", "cols", "slabs"))
    partner = {"rows": 1 - me_row}
    peers = (
        {"cols": lax.rem(me_col + cols - 1, cols)},
        {"cols": lax.rem(me_col + 1, cols)},
        {"slabs": lax.rem(me_slab + slabs - 1, slabs)},
        {"slabs": lax.rem(me_slab + 1, slabs)},
    )
    inner_x, inner_z = pl.ds(1, width), pl.ds(Z, depth)

    def load(chunk):
        return pltpu.make_async_copy(
            f_hbm.at[pl.ds(chunk * part, part)],
            field.at[0, pl.ds(1 + chunk * part, part), inner_x, inner_z],
            load_sem.at[chunk],
        )

    def load_crowd(chunk):
        part_rows = pl.ds(chunk * part, part)
        return pltpu.make_async_copy(c_hbm.at[part_rows], crowd.at[part_rows], crowd_sem.at[chunk])

    def face(slot, chunk, side):
        part_rows = pl.ds(1 + chunk * part, part)
        source, target = (
            ((1, inner_z), (width + 1, inner_z)),
            ((width, inner_z), (0, inner_z)),
            ((inner_x, Z), (inner_x, Z + depth)),
            ((inner_x, Z + depth - 1), (inner_x, Z - 1)),
        )[side]
        return pltpu.make_async_remote_copy(
            src_ref=field.at[(slot, part_rows) + source],
            dst_ref=field.at[(slot, part_rows) + target],
            send_sem=send_sem.at[slot, chunk, side],
            recv_sem=recv_sem.at[slot, chunk, side],
            device_id=peers[side],
            device_id_type=MESH,
        )

    def edge_row(slot, side):
        source, target = ((1, height + 1), (height, 0))[side]
        return pltpu.make_async_remote_copy(
            src_ref=field.at[slot, source, inner_x, inner_z],
            dst_ref=field.at[slot, target, inner_x, inner_z],
            send_sem=row_send.at[slot, side],
            recv_sem=row_recv.at[slot, side],
            device_id=partner,
            device_id_type=MESH,
        )

    def on_edges(chunk, act):
        @pl.when(chunk == 0)
        def _():
            act(0)

        @pl.when(chunk == CHUNKS - 1)
        def _():
            act(1)

    def send(slot, chunk):
        for side in range(4):
            face(slot, chunk, side).start()
        on_edges(chunk, lambda side: edge_row(slot, side).start())

    def sent(slot, chunk):
        for side in range(4):
            face(slot, chunk, side).wait_send()
        on_edges(chunk, lambda side: edge_row(slot, side).wait_send())

    def arrived(slot, chunk):
        for side in range(4):
            face(slot, chunk, side).wait_recv()
        on_edges(chunk, lambda side: edge_row(slot, 1 - side).wait_recv())

    def advance(slot, chunk, store):
        def row(step, _):
            y = chunk * part + step
            centre = [field[slot, y + 1, x, inner_z] for x in range(width + 2)]
            for x in range(width):
                value = centre[x + 1]
                around = (
                    (field[slot, y, x + 1, inner_z] + field[slot, y + 2, x + 1, inner_z])
                    + (centre[x] + centre[x + 2])
                    + (field[slot, y + 1, x + 1, pl.ds(Z - 1, depth)] + field[slot, y + 1, x + 1, pl.ds(Z + 1, depth)])
                )
                store(y, x, 0.1 * around + value * (0.6 - (0.2 * value) * crowd[y, x]))
            return 0

        lax.fori_loop(0, part, row, 0)

    for chunk in range(CHUNKS):
        load(chunk).start()
    for chunk in range(CHUNKS):
        load_crowd(chunk).start()

    barrier = pltpu.get_barrier_semaphore()
    for peer in peers + (partner,):
        pl.semaphore_signal(barrier, inc=1, device_id=peer, device_id_type=MESH)
    pl.semaphore_wait(barrier, len(peers) + 1)

    def begin(chunk, _):
        load(chunk).wait()
        send(0, chunk)
        return 0

    lax.fori_loop(0, CHUNKS, begin, 0)

    def loaded(chunk, _):
        load_crowd(chunk).wait()
        return 0

    lax.fori_loop(0, CHUNKS, loaded, 0)

    def one_step(step, _):
        slot = lax.rem(step, 2)
        other = 1 - slot

        def one_chunk(place, _):
            chunk = lax.rem(place + step, CHUNKS)
            arrived(slot, chunk)

            @pl.when(step > 0)
            def _():
                sent(other, chunk)

            def store(y, x, value):
                field[other, y + 1, x + 1, inner_z] = value

            advance(slot, chunk, store)
            send(other, chunk)
            return 0

        lax.fori_loop(0, CHUNKS, one_chunk, 0)
        return 0

    lax.fori_loop(0, STEPS - 1, one_step, 0)

    step = STEPS - 1
    slot = step % 2

    def last_chunk(place, _):
        chunk = lax.rem(place + step, CHUNKS)
        arrived(slot, chunk)

        def store(y, x, value):
            end_ref[y, x] = value

        advance(slot, chunk, store)

        @pl.when(place == 0)
        def _():
            for x in range(width):
                shift[x] = end_ref[chunk * part, x]
                first[x] = jnp.zeros_like(first[x])
                second[x] = jnp.zeros_like(second[x])

        for x in range(width):
            middle = shift[x]
            one, two = first[x], second[x]
            for y in range(part):
                moved = end_ref[chunk * part + y, x] - middle
                one, two = one + moved, two + moved * moved
            first[x], second[x] = one, two
        return 0

    lax.fori_loop(0, CHUNKS, last_chunk, 0)

    for x in range(width):
        mine[0, x] = shift[x] + first[x] * (1.0 / height)
        mine[1, x] = second[x] - first[x] * first[x] * (1.0 / height)
    swap = pltpu.make_async_remote_copy(
        src_ref=mine,
        dst_ref=theirs,
        send_sem=stat_send,
        recv_sem=stat_recv,
        device_id=partner,
        device_id_type=MESH,
    )
    swap.start()

    def drain(chunk, _):
        sent(1 - slot, chunk)
        sent(slot, chunk)
        return 0

    lax.fori_loop(0, CHUNKS, drain, 0)
    swap.wait()
    for x in range(width):
        apart = mine[0, x] - theirs[0, x]
        total = mine[1, x] + theirs[1, x] + apart * apart * (0.5 * height)
        mean_ref[x] = 0.5 * (mine[0, x] + theirs[0, x])
        scale_ref[x] = lax.rsqrt(total * (0.5 / height) + 0.0001)


def finish(end_ref, mean_ref, scale_ref, standardized_hbm, end_hbm, standardized, out_sem, end_sem):
    height, width = end_ref.shape[:2]
    part = height // CHUNKS
    copy_end = pltpu.make_async_copy(end_ref, end_hbm, end_sem)

    def copy_out(chunk):
        part_rows = pl.ds(chunk * part, part)
        return pltpu.make_async_copy(standardized.at[part_rows], standardized_hbm.at[part_rows], out_sem.at[chunk])

    copy_end.start()
    for chunk in range(CHUNKS):

        def row(step, _):
            y = chunk * part + step
            for x in range(width):
                standardized[y, x] = (end_ref[y, x] - mean_ref[x]) * scale_ref[x]
            return 0

        lax.fori_loop(0, part, row, 0)
        copy_out(chunk).start()
    for chunk in range(CHUNKS):
        copy_out(chunk).wait()
    copy_end.wait()


def local(sizes, field_values, crowding):
    height, width, depth, lanes = field_values.shape
    whole = jax.ShapeDtypeStruct(field_values.shape, jnp.float32)
    line = jax.ShapeDtypeStruct((width, depth, lanes), jnp.float32)
    vmem, anywhere = pl.BlockSpec(memory_space=pltpu.VMEM), pl.BlockSpec(memory_space=pl.ANY)
    plane = pltpu.VMEM((width, depth, lanes), jnp.float32)
    end, mean, scale = pl.pallas_call(
        functools.partial(evolve, sizes),
        out_shape=(whole, line, line),
        in_specs=[anywhere, anywhere],
        out_specs=(vmem, vmem, vmem),
        scratch_shapes=[
            pltpu.VMEM((2, height + 2, width + 2, 3 * depth, lanes), jnp.float32),
            pltpu.VMEM((height, width, depth, lanes), jnp.float32),
            plane,
            plane,
            plane,
            pltpu.VMEM((2, width, depth, lanes), jnp.float32),
            pltpu.VMEM((2, width, depth, lanes), jnp.float32),
            pltpu.SemaphoreType.DMA((CHUNKS,)),
            pltpu.SemaphoreType.DMA((CHUNKS,)),
            pltpu.SemaphoreType.DMA((2, CHUNKS, 4)),
            pltpu.SemaphoreType.DMA((2, CHUNKS, 4)),
            pltpu.SemaphoreType.DMA((2, 2)),
            pltpu.SemaphoreType.DMA((2, 2)),
            pltpu.SemaphoreType.DMA,
            pltpu.SemaphoreType.DMA,
        ],
        compiler_params=pltpu.CompilerParams(collective_id=0, has_side_effects=True),
        name="evolve",
    )(field_values, crowding)
    return pl.pallas_call(
        finish,
        out_shape=(whole, whole),
        in_specs=[vmem, vmem, vmem],
        out_specs=(anywhere, anywhere),
        scratch_shapes=[
            pltpu.VMEM((height, width, depth, lanes), jnp.float32),
            pltpu.SemaphoreType.DMA((CHUNKS,)),
            pltpu.SemaphoreType.DMA,
        ],
        name="finish",
    )(end, mean, scale)


def solution(mesh):
    spec = P(("site", "rows"), "cols", "slabs", None)
    sizes = tuple(mesh.shape[axis] for axis in ("rows", "cols", "slabs"))
    return jax.shard_map(
        functools.partial(local, sizes),
        mesh=mesh,
        in_specs=(spec, spec),
        out_specs=(spec, spec),
        check_vma=False,
    )
```

```python
import functools

import jax
import jax.numpy as jnp
from jax import lax
from jax.experimental import pallas as pl
from jax.experimental.pallas import tpu as pltpu
from jax.sharding import PartitionSpec as P

STEPS = 6
CHUNKS = 6
MESH = pl.DeviceIdType.MESH
Z = 8


def evolve(sizes, f_hbm, c_hbm, end_ref, mean_ref, scale_ref, field, crowd, shift, first, second,
           mine, theirs, load_sem, crowd_sem, send_sem, recv_sem, row_send, row_recv, stat_send, stat_recv):
    rows, cols, slabs = sizes
    height, width, depth, _ = f_hbm.shape
    part = height // CHUNKS
    me_row, me_col, me_slab = (lax.axis_index(axis) for axis in ("rows", "cols", "slabs"))
    partner = {"rows": 1 - me_row}
    peers = (
        {"cols": lax.rem(me_col + cols - 1, cols)},
        {"cols": lax.rem(me_col + 1, cols)},
        {"slabs": lax.rem(me_slab + slabs - 1, slabs)},
        {"slabs": lax.rem(me_slab + 1, slabs)},
    )
    inner_x, inner_z = pl.ds(1, width), pl.ds(Z, depth)

    def load(chunk):
        return pltpu.make_async_copy(
            f_hbm.at[pl.ds(chunk * part, part)],
            field.at[0, pl.ds(1 + chunk * part, part), inner_x, inner_z],
            load_sem.at[chunk],
        )

    def load_crowd(chunk):
        part_rows = pl.ds(chunk * part, part)
        return pltpu.make_async_copy(c_hbm.at[part_rows], crowd.at[part_rows], crowd_sem.at[chunk])

    def face(slot, chunk, side):
        part_rows = pl.ds(1 + chunk * part, part)
        source, target = (
            ((1, inner_z), (width + 1, inner_z)),
            ((width, inner_z), (0, inner_z)),
            ((inner_x, Z), (inner_x, Z + depth)),
            ((inner_x, Z + depth - 1), (inner_x, Z - 1)),
        )[side]
        return pltpu.make_async_remote_copy(
            src_ref=field.at[(slot, part_rows) + source],
            dst_ref=field.at[(slot, part_rows) + target],
            send_sem=send_sem.at[slot, chunk, side],
            recv_sem=recv_sem.at[slot, chunk, side],
            device_id=peers[side],
            device_id_type=MESH,
        )

    def edge_row(slot, side):
        source, target = ((1, height + 1), (height, 0))[side]
        return pltpu.make_async_remote_copy(
            src_ref=field.at[slot, source, inner_x, inner_z],
            dst_ref=field.at[slot, target, inner_x, inner_z],
            send_sem=row_send.at[slot, side],
            recv_sem=row_recv.at[slot, side],
            device_id=partner,
            device_id_type=MESH,
        )

    def on_edges(chunk, act):
        @pl.when(chunk == 0)
        def _():
            act(0)

        @pl.when(chunk == CHUNKS - 1)
        def _():
            act(1)

    def send(slot, chunk):
        for side in range(4):
            face(slot, chunk, side).start()
        on_edges(chunk, lambda side: edge_row(slot, side).start())

    def sent(slot, chunk):
        for side in range(4):
            face(slot, chunk, side).wait_send()
        on_edges(chunk, lambda side: edge_row(slot, side).wait_send())

    def arrived(slot, chunk):
        for side in range(4):
            face(slot, chunk, side).wait_recv()
        on_edges(chunk, lambda side: edge_row(slot, 1 - side).wait_recv())

    def advance(slot, chunk, store):
        def row(step, _):
            y = chunk * part + step
            centre = [field[slot, y + 1, x, inner_z] for x in range(width + 2)]
            values = []
            for x in range(width):
                value = centre[x + 1]
                around = (
                    (field[slot, y, x + 1, inner_z] + field[slot, y + 2, x + 1, inner_z])
                    + (centre[x] + centre[x + 2])
                    + (field[slot, y + 1, x + 1, pl.ds(Z - 1, depth)] + field[slot, y + 1, x + 1, pl.ds(Z + 1, depth)])
                )
                values.append(0.1 * around + value * (0.6 - (0.2 * value) * crowd[y, x]))
            for x in range(width):
                store(y, x, values[x])
            return 0

        lax.fori_loop(0, part, row, 0)

    for chunk in range(CHUNKS):
        load(chunk).start()
    for chunk in range(CHUNKS):
        load_crowd(chunk).start()

    barrier = pltpu.get_barrier_semaphore()
    for peer in peers + (partner,):
        pl.semaphore_signal(barrier, inc=1, device_id=peer, device_id_type=MESH)
    pl.semaphore_wait(barrier, len(peers) + 1)

    def begin(chunk, _):
        load(chunk).wait()
        send(0, chunk)
        return 0

    lax.fori_loop(0, CHUNKS, begin, 0)

    def loaded(chunk, _):
        load_crowd(chunk).wait()
        return 0

    lax.fori_loop(0, CHUNKS, loaded, 0)

    def one_step(step, _):
        slot = lax.rem(step, 2)
        other = 1 - slot

        def one_chunk(place, _):
            chunk = lax.rem(place + step, CHUNKS)
            arrived(slot, chunk)

            @pl.when(step > 0)
            def _():
                sent(other, chunk)

            def store(y, x, value):
                field[other, y + 1, x + 1, inner_z] = value

            advance(slot, chunk, store)
            send(other, chunk)
            return 0

        lax.fori_loop(0, CHUNKS, one_chunk, 0)
        return 0

    lax.fori_loop(0, STEPS - 1, one_step, 0)

    step = STEPS - 1
    slot = step % 2

    def last_chunk(place, _):
        chunk = lax.rem(place + step, CHUNKS)
        arrived(slot, chunk)

        def store(y, x, value):
            end_ref[y, x] = value

        advance(slot, chunk, store)

        @pl.when(place == 0)
        def _():
            for x in range(width):
                shift[x] = end_ref[chunk * part, x]
                first[x] = jnp.zeros_like(first[x])
                second[x] = jnp.zeros_like(second[x])

        for x in range(width):
            middle = shift[x]
            one, two = first[x], second[x]
            for y in range(part):
                moved = end_ref[chunk * part + y, x] - middle
                one, two = one + moved, two + moved * moved
            first[x], second[x] = one, two
        return 0

    lax.fori_loop(0, CHUNKS, last_chunk, 0)

    for x in range(width):
        mine[0, x] = shift[x] + first[x] * (1.0 / height)
        mine[1, x] = second[x] - first[x] * first[x] * (1.0 / height)
    swap = pltpu.make_async_remote_copy(
        src_ref=mine,
        dst_ref=theirs,
        send_sem=stat_send,
        recv_sem=stat_recv,
        device_id=partner,
        device_id_type=MESH,
    )
    swap.start()

    def drain(chunk, _):
        sent(1 - slot, chunk)
        sent(slot, chunk)
        return 0

    lax.fori_loop(0, CHUNKS, drain, 0)
    swap.wait()
    for x in range(width):
        apart = mine[0, x] - theirs[0, x]
        total = mine[1, x] + theirs[1, x] + apart * apart * (0.5 * height)
        mean_ref[x] = 0.5 * (mine[0, x] + theirs[0, x])
        scale_ref[x] = lax.rsqrt(total * (0.5 / height) + 0.0001)


def finish(end_ref, mean_ref, scale_ref, standardized_hbm, end_hbm, standardized, out_sem, end_sem):
    height, width = end_ref.shape[:2]
    part = height // CHUNKS
    copy_end = pltpu.make_async_copy(end_ref, end_hbm, end_sem)

    def copy_out(chunk):
        part_rows = pl.ds(chunk * part, part)
        return pltpu.make_async_copy(standardized.at[part_rows], standardized_hbm.at[part_rows], out_sem.at[chunk])

    copy_end.start()
    for chunk in range(CHUNKS):

        def row(step, _):
            y = chunk * part + step
            for x in range(width):
                standardized[y, x] = (end_ref[y, x] - mean_ref[x]) * scale_ref[x]
            return 0

        lax.fori_loop(0, part, row, 0)
        copy_out(chunk).start()
    for chunk in range(CHUNKS):
        copy_out(chunk).wait()
    copy_end.wait()


def local(sizes, field_values, crowding):
    height, width, depth, lanes = field_values.shape
    whole = jax.ShapeDtypeStruct(field_values.shape, jnp.float32)
    line = jax.ShapeDtypeStruct((width, depth, lanes), jnp.float32)
    vmem, anywhere = pl.BlockSpec(memory_space=pltpu.VMEM), pl.BlockSpec(memory_space=pl.ANY)
    plane = pltpu.VMEM((width, depth, lanes), jnp.float32)
    end, mean, scale = pl.pallas_call(
        functools.partial(evolve, sizes),
        out_shape=tuple(pltpu.VMEM(kind.shape, jnp.float32) for kind in (whole, line, line)),
        in_specs=[anywhere, anywhere],
        out_specs=(vmem, vmem, vmem),
        scratch_shapes=[
            pltpu.VMEM((2, height + 2, width + 2, 3 * depth, lanes), jnp.float32),
            pltpu.VMEM((height, width, depth, lanes), jnp.float32),
            plane,
            plane,
            plane,
            pltpu.VMEM((2, width, depth, lanes), jnp.float32),
            pltpu.VMEM((2, width, depth, lanes), jnp.float32),
            pltpu.SemaphoreType.DMA((CHUNKS,)),
            pltpu.SemaphoreType.DMA((CHUNKS,)),
            pltpu.SemaphoreType.DMA((2, CHUNKS, 4)),
            pltpu.SemaphoreType.DMA((2, CHUNKS, 4)),
            pltpu.SemaphoreType.DMA((2, 2)),
            pltpu.SemaphoreType.DMA((2, 2)),
            pltpu.SemaphoreType.DMA,
            pltpu.SemaphoreType.DMA,
        ],
        compiler_params=pltpu.CompilerParams(collective_id=0, has_side_effects=True),
        name="evolve",
    )(field_values, crowding)
    return pl.pallas_call(
        finish,
        out_shape=(whole, whole),
        in_specs=[vmem, vmem, vmem],
        out_specs=(anywhere, anywhere),
        scratch_shapes=[
            pltpu.VMEM((height, width, depth, lanes), jnp.float32),
            pltpu.SemaphoreType.DMA((CHUNKS,)),
            pltpu.SemaphoreType.DMA,
        ],
        name="finish",
    )(*(pltpu.with_memory_space_constraint(value, pltpu.VMEM) for value in (end, mean, scale)))


def solution(mesh):
    spec = P(("site", "rows"), "cols", "slabs", None)
    sizes = tuple(mesh.shape[axis] for axis in ("rows", "cols", "slabs"))
    return jax.shard_map(
        functools.partial(local, sizes),
        mesh=mesh,
        in_specs=(spec, spec),
        out_specs=(spec, spec),
        check_vma=False,
    )
```

```python
import functools

import jax
import jax.numpy as jnp
from jax import lax
from jax.experimental import pallas as pl
from jax.experimental.pallas import tpu as pltpu
from jax.sharding import PartitionSpec as P

STEPS = 6
CHUNKS = 6
MESH = pl.DeviceIdType.MESH
Z = 8


def evolve(sizes, f_hbm, c_hbm, end_ref, mine, theirs, field, crowd, shift, first, second, load_sem, crowd_sem,
           send_sem, recv_sem, row_send, row_recv, stat_send, stat_recv):
    rows, cols, slabs = sizes
    height, width, depth, _ = f_hbm.shape
    part = height // CHUNKS
    me_row, me_col, me_slab = (lax.axis_index(axis) for axis in ("rows", "cols", "slabs"))
    partner = {"rows": 1 - me_row}
    peers = (
        {"cols": lax.rem(me_col + cols - 1, cols)},
        {"cols": lax.rem(me_col + 1, cols)},
        {"slabs": lax.rem(me_slab + slabs - 1, slabs)},
        {"slabs": lax.rem(me_slab + 1, slabs)},
    )
    inner_x, inner_z = pl.ds(1, width), pl.ds(Z, depth)

    def load(chunk):
        return pltpu.make_async_copy(
            f_hbm.at[pl.ds(chunk * part, part)],
            field.at[0, pl.ds(1 + chunk * part, part), inner_x, inner_z],
            load_sem.at[chunk],
        )

    def load_crowd(chunk):
        part_rows = pl.ds(chunk * part, part)
        return pltpu.make_async_copy(c_hbm.at[part_rows], crowd.at[part_rows], crowd_sem.at[chunk])

    def face(slot, chunk, side):
        part_rows = pl.ds(1 + chunk * part, part)
        source, target = (
            ((1, inner_z), (width + 1, inner_z)),
            ((width, inner_z), (0, inner_z)),
            ((inner_x, Z), (inner_x, Z + depth)),
            ((inner_x, Z + depth - 1), (inner_x, Z - 1)),
        )[side]
        return pltpu.make_async_remote_copy(
            src_ref=field.at[(slot, part_rows) + source],
            dst_ref=field.at[(slot, part_rows) + target],
            send_sem=send_sem.at[slot, chunk, side],
            recv_sem=recv_sem.at[slot, chunk, side],
            device_id=peers[side],
            device_id_type=MESH,
        )

    def edge_row(slot, side):
        source, target = ((1, height + 1), (height, 0))[side]
        return pltpu.make_async_remote_copy(
            src_ref=field.at[slot, source, inner_x, inner_z],
            dst_ref=field.at[slot, target, inner_x, inner_z],
            send_sem=row_send.at[slot, side],
            recv_sem=row_recv.at[slot, side],
            device_id=partner,
            device_id_type=MESH,
        )

    def on_edges(chunk, act):
        @pl.when(chunk == 0)
        def _():
            act(0)

        @pl.when(chunk == CHUNKS - 1)
        def _():
            act(1)

    def send(slot, chunk):
        for side in range(4):
            face(slot, chunk, side).start()
        on_edges(chunk, lambda side: edge_row(slot, side).start())

    def sent(slot, chunk):
        for side in range(4):
            face(slot, chunk, side).wait_send()
        on_edges(chunk, lambda side: edge_row(slot, side).wait_send())

    def arrived(slot, chunk):
        for side in range(4):
            face(slot, chunk, side).wait_recv()
        on_edges(chunk, lambda side: edge_row(slot, 1 - side).wait_recv())

    def advance(slot, chunk, store):
        def row(step, _):
            y = chunk * part + step
            centre = [field[slot, y + 1, x, inner_z] for x in range(width + 2)]
            values = []
            for x in range(width):
                value = centre[x + 1]
                around = (
                    (field[slot, y, x + 1, inner_z] + field[slot, y + 2, x + 1, inner_z])
                    + (centre[x] + centre[x + 2])
                    + (field[slot, y + 1, x + 1, pl.ds(Z - 1, depth)] + field[slot, y + 1, x + 1, pl.ds(Z + 1, depth)])
                )
                values.append(0.1 * around + value * (0.6 - (0.2 * value) * crowd[y, x]))
            for x in range(width):
                store(y, x, values[x])
            return 0

        lax.fori_loop(0, part, row, 0)

    barrier = pltpu.get_barrier_semaphore()
    for peer in peers + (partner,):
        pl.semaphore_signal(barrier, inc=1, device_id=peer, device_id_type=MESH)
    for chunk in range(CHUNKS):
        load(chunk).start()
    pl.semaphore_wait(barrier, len(peers) + 1)

    def begin(chunk, _):
        load(chunk).wait()
        send(0, chunk)
        return 0

    lax.fori_loop(0, CHUNKS, begin, 0)
    for chunk in range(CHUNKS):
        load_crowd(chunk).start()

    def loaded(chunk, _):
        load_crowd(chunk).wait()
        return 0

    lax.fori_loop(0, CHUNKS, loaded, 0)

    def one_step(step, _):
        slot = lax.rem(step, 2)
        other = 1 - slot

        def one_chunk(place, _):
            chunk = lax.rem(place + step, CHUNKS)
            arrived(slot, chunk)

            @pl.when(step > 0)
            def _():
                sent(other, chunk)

            def store(y, x, value):
                field[other, y + 1, x + 1, inner_z] = value

            advance(slot, chunk, store)
            send(other, chunk)
            return 0

        lax.fori_loop(0, CHUNKS, one_chunk, 0)
        return 0

    lax.fori_loop(0, STEPS - 1, one_step, 0)

    step = STEPS - 1
    slot = step % 2

    def last_chunk(place, _):
        chunk = lax.rem(place + step, CHUNKS)
        arrived(slot, chunk)

        def store(y, x, value):
            end_ref[y, x] = value

        advance(slot, chunk, store)

        @pl.when(place == 0)
        def _():
            for x in range(width):
                shift[x] = end_ref[chunk * part, x]
                first[x] = jnp.zeros_like(first[x])
                second[x] = jnp.zeros_like(second[x])

        for x in range(width):
            middle = shift[x]
            one, two = first[x], second[x]
            for y in range(part):
                moved = end_ref[chunk * part + y, x] - middle
                one, two = one + moved, two + moved * moved
            first[x], second[x] = one, two
        return 0

    lax.fori_loop(0, CHUNKS, last_chunk, 0)

    for x in range(width):
        mine[0, x] = shift[x] + first[x] * (1.0 / height)
        mine[1, x] = second[x] - first[x] * first[x] * (1.0 / height)
    swap = pltpu.make_async_remote_copy(
        src_ref=mine,
        dst_ref=theirs,
        send_sem=stat_send,
        recv_sem=stat_recv,
        device_id=partner,
        device_id_type=MESH,
    )
    swap.start()

    def drain(chunk, _):
        sent(1 - slot, chunk)
        sent(slot, chunk)
        return 0

    lax.fori_loop(0, CHUNKS, drain, 0)
    swap.wait()


def finish(end_ref, mine, theirs, standardized_hbm, end_hbm, standardized, mean_ref, scale_ref, out_sem, end_sem):
    height, width = end_ref.shape[:2]
    part = height // CHUNKS

    def copy_end(chunk):
        part_rows = pl.ds(chunk * part, part)
        return pltpu.make_async_copy(end_ref.at[part_rows], end_hbm.at[part_rows], end_sem.at[chunk])

    def copy_out(chunk):
        part_rows = pl.ds(chunk * part, part)
        return pltpu.make_async_copy(standardized.at[part_rows], standardized_hbm.at[part_rows], out_sem.at[chunk])

    for chunk in range(CHUNKS):
        copy_end(chunk).start()
    for x in range(width):
        apart = mine[0, x] - theirs[0, x]
        total = mine[1, x] + theirs[1, x] + apart * apart * (0.5 * height)
        mean_ref[x] = 0.5 * (mine[0, x] + theirs[0, x])
        scale_ref[x] = lax.rsqrt(total * (0.5 / height) + 0.0001)
    for chunk in range(CHUNKS):

        def row(step, _):
            y = chunk * part + step
            for x in range(width):
                standardized[y, x] = (end_ref[y, x] - mean_ref[x]) * scale_ref[x]
            return 0

        lax.fori_loop(0, part, row, 0)
        copy_out(chunk).start()
    for chunk in range(CHUNKS):
        copy_out(chunk).wait()
    for chunk in range(CHUNKS):
        copy_end(chunk).wait()


def local(sizes, field_values, crowding):
    height, width, depth, lanes = field_values.shape
    whole = jax.ShapeDtypeStruct(field_values.shape, jnp.float32)
    pair = jax.ShapeDtypeStruct((2, width, depth, lanes), jnp.float32)
    vmem, anywhere = pl.BlockSpec(memory_space=pltpu.VMEM), pl.BlockSpec(memory_space=pl.ANY)
    plane = pltpu.VMEM((width, depth, lanes), jnp.float32)
    end, mine, theirs = pl.pallas_call(
        functools.partial(evolve, sizes),
        out_shape=tuple(pltpu.VMEM(kind.shape, jnp.float32) for kind in (whole, pair, pair)),
        in_specs=[anywhere, anywhere],
        out_specs=(vmem, vmem, vmem),
        scratch_shapes=[
            pltpu.VMEM((2, height + 2, width + 2, 3 * depth, lanes), jnp.float32),
            pltpu.VMEM((height, width, depth, lanes), jnp.float32),
            plane,
            plane,
            plane,
            pltpu.SemaphoreType.DMA((CHUNKS,)),
            pltpu.SemaphoreType.DMA((CHUNKS,)),
            pltpu.SemaphoreType.DMA((2, CHUNKS, 4)),
            pltpu.SemaphoreType.DMA((2, CHUNKS, 4)),
            pltpu.SemaphoreType.DMA((2, 2)),
            pltpu.SemaphoreType.DMA((2, 2)),
            pltpu.SemaphoreType.DMA,
            pltpu.SemaphoreType.DMA,
        ],
        compiler_params=pltpu.CompilerParams(collective_id=0, has_side_effects=True),
        name="evolve",
    )(field_values, crowding)
    return pl.pallas_call(
        finish,
        out_shape=(whole, whole),
        in_specs=[vmem, vmem, vmem],
        out_specs=(anywhere, anywhere),
        scratch_shapes=[
            pltpu.VMEM((height, width, depth, lanes), jnp.float32),
            plane,
            plane,
            pltpu.SemaphoreType.DMA((CHUNKS,)),
            pltpu.SemaphoreType.DMA((CHUNKS,)),
        ],
        name="finish",
    )(*(pltpu.with_memory_space_constraint(value, pltpu.VMEM) for value in (end, mine, theirs)))


def solution(mesh):
    spec = P(("site", "rows"), "cols", "slabs", None)
    sizes = tuple(mesh.shape[axis] for axis in ("rows", "cols", "slabs"))
    return jax.shard_map(
        functools.partial(local, sizes),
        mesh=mesh,
        in_specs=(spec, spec),
        out_specs=(spec, spec),
        check_vma=False,
    )
```

```python
import functools

import jax
import jax.numpy as jnp
from jax import lax
from jax.experimental import pallas as pl
from jax.experimental.pallas import tpu as pltpu
from jax.sharding import PartitionSpec as P

STEPS = 6
CHUNKS = 6
MESH = pl.DeviceIdType.MESH
Z = 8


def evolve(sizes, f_hbm, c_hbm, end_ref, mine, theirs, field, crowd, shift, first, second, load_sem, crowd_sem,
           send_sem, recv_sem, row_send, row_recv, stat_send, stat_recv):
    rows, cols, slabs = sizes
    height, width, depth, _ = f_hbm.shape
    part = height // CHUNKS
    me_row, me_col, me_slab = (lax.axis_index(axis) for axis in ("rows", "cols", "slabs"))
    partner = {"rows": 1 - me_row}
    peers = (
        {"cols": lax.rem(me_col + cols - 1, cols)},
        {"cols": lax.rem(me_col + 1, cols)},
        {"slabs": lax.rem(me_slab + slabs - 1, slabs)},
        {"slabs": lax.rem(me_slab + 1, slabs)},
    )
    inner_x, inner_z = pl.ds(1, width), pl.ds(Z, depth)

    def load(chunk):
        return pltpu.make_async_copy(
            f_hbm.at[pl.ds(chunk * part, part)],
            field.at[0, pl.ds(1 + chunk * part, part), inner_x, inner_z],
            load_sem.at[chunk],
        )

    def load_crowd(chunk):
        part_rows = pl.ds(chunk * part, part)
        return pltpu.make_async_copy(c_hbm.at[part_rows], crowd.at[part_rows], crowd_sem.at[chunk])

    def face(slot, chunk, side):
        part_rows = pl.ds(1 + chunk * part, part)
        source, target = (
            ((1, inner_z), (width + 1, inner_z)),
            ((width, inner_z), (0, inner_z)),
            ((inner_x, Z), (inner_x, Z + depth)),
            ((inner_x, Z + depth - 1), (inner_x, Z - 1)),
        )[side]
        return pltpu.make_async_remote_copy(
            src_ref=field.at[(slot, part_rows) + source],
            dst_ref=field.at[(slot, part_rows) + target],
            send_sem=send_sem.at[slot, chunk, side],
            recv_sem=recv_sem.at[slot, chunk, side],
            device_id=peers[side],
            device_id_type=MESH,
        )

    def edge_row(slot, side):
        source, target = ((1, height + 1), (height, 0))[side]
        return pltpu.make_async_remote_copy(
            src_ref=field.at[slot, source, inner_x, inner_z],
            dst_ref=field.at[slot, target, inner_x, inner_z],
            send_sem=row_send.at[slot, side],
            recv_sem=row_recv.at[slot, side],
            device_id=partner,
            device_id_type=MESH,
        )

    def on_edges(chunk, act):
        @pl.when(chunk == 0)
        def _():
            act(0)

        @pl.when(chunk == CHUNKS - 1)
        def _():
            act(1)

    def send(slot, chunk):
        for side in range(4):
            face(slot, chunk, side).start()
        on_edges(chunk, lambda side: edge_row(slot, side).start())

    def sent(slot, chunk):
        for side in range(4):
            face(slot, chunk, side).wait_send()
        on_edges(chunk, lambda side: edge_row(slot, side).wait_send())

    def arrived(slot, chunk):
        for side in range(4):
            face(slot, chunk, side).wait_recv()
        on_edges(chunk, lambda side: edge_row(slot, 1 - side).wait_recv())

    def advance(slot, chunk, store):
        def row(step, _):
            y = chunk * part + step
            centre = [field[slot, y + 1, x, inner_z] for x in range(width + 2)]
            values = []
            for x in range(width):
                value = centre[x + 1]
                around = (
                    (field[slot, y, x + 1, inner_z] + field[slot, y + 2, x + 1, inner_z])
                    + (centre[x] + centre[x + 2])
                    + (field[slot, y + 1, x + 1, pl.ds(Z - 1, depth)] + field[slot, y + 1, x + 1, pl.ds(Z + 1, depth)])
                )
                values.append(0.1 * around + value * (0.6 - (0.2 * value) * crowd[y, x]))
            for x in range(width):
                store(y, x, values[x])
            return 0

        lax.fori_loop(0, part, row, 0)

    barrier = pltpu.get_barrier_semaphore()
    for peer in peers + (partner,):
        pl.semaphore_signal(barrier, inc=1, device_id=peer, device_id_type=MESH)
    for chunk in range(CHUNKS):
        load(chunk).start()
    pl.semaphore_wait(barrier, len(peers) + 1)

    def begin(chunk, _):
        load(chunk).wait()
        send(0, chunk)
        return 0

    lax.fori_loop(0, CHUNKS, begin, 0)
    for chunk in range(CHUNKS):
        load_crowd(chunk).start()

    def loaded(chunk, _):
        load_crowd(chunk).wait()
        return 0

    lax.fori_loop(0, CHUNKS, loaded, 0)

    def one_step(step, _):
        slot = lax.rem(step, 2)
        other = 1 - slot

        def one_chunk(place, _):
            chunk = place
            arrived(slot, chunk)

            @pl.when(step > 0)
            def _():
                sent(other, chunk)

            def store(y, x, value):
                field[other, y + 1, x + 1, inner_z] = value

            advance(slot, chunk, store)
            send(other, chunk)
            return 0

        lax.fori_loop(0, CHUNKS, one_chunk, 0)
        return 0

    lax.fori_loop(0, STEPS - 1, one_step, 0)

    step = STEPS - 1
    slot = step % 2

    def last_chunk(place, _):
        chunk = place
        arrived(slot, chunk)

        def store(y, x, value):
            end_ref[y, x] = value

        advance(slot, chunk, store)

        @pl.when(place == 0)
        def _():
            for x in range(width):
                shift[x] = end_ref[chunk * part, x]
                first[x] = jnp.zeros_like(first[x])
                second[x] = jnp.zeros_like(second[x])

        for x in range(width):
            middle = shift[x]
            one, two = first[x], second[x]
            for y in range(part):
                moved = end_ref[chunk * part + y, x] - middle
                one, two = one + moved, two + moved * moved
            first[x], second[x] = one, two
        return 0

    lax.fori_loop(0, CHUNKS, last_chunk, 0)

    for x in range(width):
        mine[0, x] = shift[x] + first[x] * (1.0 / height)
        mine[1, x] = second[x] - first[x] * first[x] * (1.0 / height)
    swap = pltpu.make_async_remote_copy(
        src_ref=mine,
        dst_ref=theirs,
        send_sem=stat_send,
        recv_sem=stat_recv,
        device_id=partner,
        device_id_type=MESH,
    )
    swap.start()

    def drain(chunk, _):
        sent(1 - slot, chunk)
        sent(slot, chunk)
        return 0

    lax.fori_loop(0, CHUNKS, drain, 0)
    swap.wait()


def finish(end_ref, mine, theirs, standardized_hbm, end_hbm, standardized, mean_ref, scale_ref, out_sem, end_sem):
    height, width = end_ref.shape[:2]
    part = height // CHUNKS

    def copy_end(chunk):
        part_rows = pl.ds(chunk * part, part)
        return pltpu.make_async_copy(end_ref.at[part_rows], end_hbm.at[part_rows], end_sem.at[chunk])

    def copy_out(chunk):
        part_rows = pl.ds(chunk * part, part)
        return pltpu.make_async_copy(standardized.at[part_rows], standardized_hbm.at[part_rows], out_sem.at[chunk])

    for chunk in range(CHUNKS):
        copy_end(chunk).start()
    for x in range(width):
        apart = mine[0, x] - theirs[0, x]
        total = mine[1, x] + theirs[1, x] + apart * apart * (0.5 * height)
        mean_ref[x] = 0.5 * (mine[0, x] + theirs[0, x])
        scale_ref[x] = lax.rsqrt(total * (0.5 / height) + 0.0001)
    for chunk in range(CHUNKS):

        def row(step, _):
            y = chunk * part + step
            for x in range(width):
                standardized[y, x] = (end_ref[y, x] - mean_ref[x]) * scale_ref[x]
            return 0

        lax.fori_loop(0, part, row, 0)
        copy_out(chunk).start()
    for chunk in range(CHUNKS):
        copy_out(chunk).wait()
    for chunk in range(CHUNKS):
        copy_end(chunk).wait()


def local(sizes, field_values, crowding):
    height, width, depth, lanes = field_values.shape
    whole = jax.ShapeDtypeStruct(field_values.shape, jnp.float32)
    pair = jax.ShapeDtypeStruct((2, width, depth, lanes), jnp.float32)
    vmem, anywhere = pl.BlockSpec(memory_space=pltpu.VMEM), pl.BlockSpec(memory_space=pl.ANY)
    plane = pltpu.VMEM((width, depth, lanes), jnp.float32)
    end, mine, theirs = pl.pallas_call(
        functools.partial(evolve, sizes),
        out_shape=tuple(pltpu.VMEM(kind.shape, jnp.float32) for kind in (whole, pair, pair)),
        in_specs=[anywhere, anywhere],
        out_specs=(vmem, vmem, vmem),
        scratch_shapes=[
            pltpu.VMEM((2, height + 2, width + 2, 3 * depth, lanes), jnp.float32),
            pltpu.VMEM((height, width, depth, lanes), jnp.float32),
            plane,
            plane,
            plane,
            pltpu.SemaphoreType.DMA((CHUNKS,)),
            pltpu.SemaphoreType.DMA((CHUNKS,)),
            pltpu.SemaphoreType.DMA((2, CHUNKS, 4)),
            pltpu.SemaphoreType.DMA((2, CHUNKS, 4)),
            pltpu.SemaphoreType.DMA((2, 2)),
            pltpu.SemaphoreType.DMA((2, 2)),
            pltpu.SemaphoreType.DMA,
            pltpu.SemaphoreType.DMA,
        ],
        compiler_params=pltpu.CompilerParams(collective_id=0, has_side_effects=True),
        name="evolve",
    )(field_values, crowding)
    return pl.pallas_call(
        finish,
        out_shape=(whole, whole),
        in_specs=[vmem, vmem, vmem],
        out_specs=(anywhere, anywhere),
        scratch_shapes=[
            pltpu.VMEM((height, width, depth, lanes), jnp.float32),
            plane,
            plane,
            pltpu.SemaphoreType.DMA((CHUNKS,)),
            pltpu.SemaphoreType.DMA((CHUNKS,)),
        ],
        name="finish",
    )(*(pltpu.with_memory_space_constraint(value, pltpu.VMEM) for value in (end, mine, theirs)))


def solution(mesh):
    spec = P(("site", "rows"), "cols", "slabs", None)
    sizes = tuple(mesh.shape[axis] for axis in ("rows", "cols", "slabs"))
    return jax.shard_map(
        functools.partial(local, sizes),
        mesh=mesh,
        in_specs=(spec, spec),
        out_specs=(spec, spec),
        check_vma=False,
    )
```

```python
import functools

import jax
import jax.numpy as jnp
from jax import lax
from jax.experimental import pallas as pl
from jax.experimental.pallas import tpu as pltpu
from jax.sharding import PartitionSpec as P

STEPS = 6
CHUNKS = 6
MESH = pl.DeviceIdType.MESH
Z = 8


def evolve(sizes, f_hbm, c_hbm, end_ref, mine, theirs, field, crowd, shift, first, second,
           send_sem, recv_sem, row_send, row_recv, stat_send, stat_recv):
    rows, cols, slabs = sizes
    height, width, depth, _ = f_hbm.shape
    part = height // CHUNKS
    me_row, me_col, me_slab = (lax.axis_index(axis) for axis in ("rows", "cols", "slabs"))
    partner = {"rows": 1 - me_row}
    peers = (
        {"cols": lax.rem(me_col + cols - 1, cols)},
        {"cols": lax.rem(me_col + 1, cols)},
        {"slabs": lax.rem(me_slab + slabs - 1, slabs)},
        {"slabs": lax.rem(me_slab + 1, slabs)},
    )
    inner_x, inner_z = pl.ds(1, width), pl.ds(Z, depth)

    def load(chunk):
        return pltpu.make_async_copy(
            f_hbm.at[pl.ds(chunk * part, part)],
            field.at[0, pl.ds(1 + chunk * part, part), inner_x, inner_z],
            send_sem.at[1, chunk],
        )

    def load_crowd(chunk):
        part_rows = pl.ds(chunk * part, part)
        return pltpu.make_async_copy(c_hbm.at[part_rows], crowd.at[part_rows], send_sem.at[1, chunk])

    def face(slot, chunk, side):
        part_rows = pl.ds(1 + chunk * part, part)
        source, target = (
            ((1, inner_z), (width + 1, inner_z)),
            ((width, inner_z), (0, inner_z)),
            ((inner_x, Z), (inner_x, Z + depth)),
            ((inner_x, Z + depth - 1), (inner_x, Z - 1)),
        )[side]
        return pltpu.make_async_remote_copy(
            src_ref=field.at[(slot, part_rows) + source],
            dst_ref=field.at[(slot, part_rows) + target],
            send_sem=send_sem.at[slot, chunk],
            recv_sem=recv_sem.at[slot, chunk],
            device_id=peers[side],
            device_id_type=MESH,
        )

    def edge_row(slot, side):
        source, target = ((1, height + 1), (height, 0))[side]
        return pltpu.make_async_remote_copy(
            src_ref=field.at[slot, source, inner_x, inner_z],
            dst_ref=field.at[slot, target, inner_x, inner_z],
            send_sem=row_send.at[slot, side],
            recv_sem=row_recv.at[slot, side],
            device_id=partner,
            device_id_type=MESH,
        )

    def on_edges(chunk, act):
        @pl.when(chunk == 0)
        def _():
            act(0)

        @pl.when(chunk == CHUNKS - 1)
        def _():
            act(1)

    def send(slot, chunk):
        for side in range(4):
            face(slot, chunk, side).start()
        on_edges(chunk, lambda side: edge_row(slot, side).start())

    def wait_faces(sem):
        four_faces = crowd.at[pl.ds(0, part * 2 * (width + depth) // (width * depth))]
        pltpu.make_async_copy(four_faces, four_faces, sem).wait()

    def sent(slot, chunk):
        wait_faces(send_sem.at[slot, chunk])
        on_edges(chunk, lambda side: edge_row(slot, side).wait_send())

    def arrived(slot, chunk):
        wait_faces(recv_sem.at[slot, chunk])
        on_edges(chunk, lambda side: edge_row(slot, 1 - side).wait_recv())

    def advance(slot, chunk, store):
        def row(step, _):
            y = chunk * part + step
            centre = [field[slot, y + 1, x, inner_z] for x in range(width + 2)]
            values = []
            for x in range(width):
                value = centre[x + 1]
                around = (
                    (field[slot, y, x + 1, inner_z] + field[slot, y + 2, x + 1, inner_z])
                    + (centre[x] + centre[x + 2])
                    + (field[slot, y + 1, x + 1, pl.ds(Z - 1, depth)] + field[slot, y + 1, x + 1, pl.ds(Z + 1, depth)])
                )
                values.append(0.1 * around + value * (0.6 - (0.2 * value) * crowd[y, x]))
            for x in range(width):
                store(y, x, values[x])
            return 0

        lax.fori_loop(0, part, row, 0)

    barrier = pltpu.get_barrier_semaphore()
    for peer in peers + (partner,):
        pl.semaphore_signal(barrier, inc=1, device_id=peer, device_id_type=MESH)
    for chunk in range(CHUNKS):
        load(chunk).start()
    pl.semaphore_wait(barrier, len(peers) + 1)

    def begin(chunk, _):
        load(chunk).wait()
        send(0, chunk)
        return 0

    lax.fori_loop(0, CHUNKS, begin, 0)
    for chunk in range(CHUNKS):
        load_crowd(chunk).start()

    def loaded(chunk, _):
        load_crowd(chunk).wait()
        return 0

    lax.fori_loop(0, CHUNKS, loaded, 0)

    def one_step(step, _):
        slot = lax.rem(step, 2)
        other = 1 - slot

        def one_chunk(place, _):
            chunk = place
            arrived(slot, chunk)

            @pl.when(step > 0)
            def _():
                sent(other, chunk)

            def store(y, x, value):
                field[other, y + 1, x + 1, inner_z] = value

            advance(slot, chunk, store)
            send(other, chunk)
            return 0

        lax.fori_loop(0, CHUNKS, one_chunk, 0)
        return 0

    lax.fori_loop(0, STEPS - 1, one_step, 0)

    step = STEPS - 1
    slot = step % 2

    def last_chunk(place, _):
        chunk = place
        arrived(slot, chunk)

        def store(y, x, value):
            end_ref[y, x] = value

        advance(slot, chunk, store)

        @pl.when(place == 0)
        def _():
            for x in range(width):
                shift[x] = end_ref[chunk * part, x]
                first[x] = jnp.zeros_like(first[x])
                second[x] = jnp.zeros_like(second[x])

        for x in range(width):
            middle = shift[x]
            one, two = first[x], second[x]
            for y in range(part):
                moved = end_ref[chunk * part + y, x] - middle
                one, two = one + moved, two + moved * moved
            first[x], second[x] = one, two
        return 0

    lax.fori_loop(0, CHUNKS, last_chunk, 0)

    for x in range(width):
        mine[0, x] = shift[x] + first[x] * (1.0 / height)
        mine[1, x] = second[x] - first[x] * first[x] * (1.0 / height)
    swap = pltpu.make_async_remote_copy(
        src_ref=mine,
        dst_ref=theirs,
        send_sem=stat_send,
        recv_sem=stat_recv,
        device_id=partner,
        device_id_type=MESH,
    )
    swap.start()

    def drain(chunk, _):
        sent(1 - slot, chunk)
        sent(slot, chunk)
        return 0

    lax.fori_loop(0, CHUNKS, drain, 0)
    swap.wait()


def finish(end_ref, mine, theirs, standardized_hbm, end_hbm, standardized, mean_ref, scale_ref, out_sem, end_sem):
    height, width = end_ref.shape[:2]
    part = height // CHUNKS

    copy_end = pltpu.make_async_copy(end_ref, end_hbm, end_sem)

    def copy_out(chunk):
        part_rows = pl.ds(chunk * part, part)
        return pltpu.make_async_copy(standardized.at[part_rows], standardized_hbm.at[part_rows], out_sem)

    copy_end.start()
    for x in range(width):
        apart = mine[0, x] - theirs[0, x]
        total = mine[1, x] + theirs[1, x] + apart * apart * (0.5 * height)
        mean_ref[x] = 0.5 * (mine[0, x] + theirs[0, x])
        scale_ref[x] = lax.rsqrt(total * (0.5 / height) + 0.0001)
    for chunk in range(CHUNKS):

        def row(step, _):
            y = chunk * part + step
            for x in range(width):
                standardized[y, x] = (end_ref[y, x] - mean_ref[x]) * scale_ref[x]
            return 0

        lax.fori_loop(0, part, row, 0)
        copy_out(chunk).start()
    pltpu.make_async_copy(standardized, standardized_hbm, out_sem).wait()
    copy_end.wait()


def local(sizes, field_values, crowding):
    height, width, depth, lanes = field_values.shape
    whole = jax.ShapeDtypeStruct(field_values.shape, jnp.float32)
    pair = jax.ShapeDtypeStruct((2, width, depth, lanes), jnp.float32)
    vmem, anywhere = pl.BlockSpec(memory_space=pltpu.VMEM), pl.BlockSpec(memory_space=pl.ANY)
    plane = pltpu.VMEM((width, depth, lanes), jnp.float32)
    end, mine, theirs = pl.pallas_call(
        functools.partial(evolve, sizes),
        out_shape=tuple(pltpu.VMEM(kind.shape, jnp.float32) for kind in (whole, pair, pair)),
        in_specs=[anywhere, anywhere],
        out_specs=(vmem, vmem, vmem),
        scratch_shapes=[
            pltpu.VMEM((2, height + 2, width + 2, 3 * depth, lanes), jnp.float32),
            pltpu.VMEM((height, width, depth, lanes), jnp.float32),
            plane,
            plane,
            plane,
            pltpu.SemaphoreType.DMA((2, CHUNKS)),
            pltpu.SemaphoreType.DMA((2, CHUNKS)),
            pltpu.SemaphoreType.DMA((2, 2)),
            pltpu.SemaphoreType.DMA((2, 2)),
            pltpu.SemaphoreType.DMA,
            pltpu.SemaphoreType.DMA,
        ],
        compiler_params=pltpu.CompilerParams(collective_id=0, has_side_effects=True),
        name="evolve",
    )(field_values, crowding)
    return pl.pallas_call(
        finish,
        out_shape=(whole, whole),
        in_specs=[vmem, vmem, vmem],
        out_specs=(anywhere, anywhere),
        scratch_shapes=[
            pltpu.VMEM((height, width, depth, lanes), jnp.float32),
            plane,
            plane,
            pltpu.SemaphoreType.DMA,
            pltpu.SemaphoreType.DMA,
        ],
        name="finish",
    )(*(pltpu.with_memory_space_constraint(value, pltpu.VMEM) for value in (end, mine, theirs)))


def solution(mesh):
    spec = P(("site", "rows"), "cols", "slabs", None)
    sizes = tuple(mesh.shape[axis] for axis in ("rows", "cols", "slabs"))
    return jax.shard_map(
        functools.partial(local, sizes),
        mesh=mesh,
        in_specs=(spec, spec),
        out_specs=(spec, spec),
        check_vma=False,
    )
```

```python
import functools

import jax
import jax.numpy as jnp
from jax import lax
from jax.experimental import pallas as pl
from jax.experimental.pallas import tpu as pltpu
from jax.sharding import PartitionSpec as P

STEPS = 6
CHUNKS = 12
MESH = pl.DeviceIdType.MESH
Z = 8


def evolve(sizes, f_hbm, c_hbm, end_ref, mine, theirs, field, crowd, shift, first, second,
           send_sem, recv_sem, row_send, row_recv, stat_send, stat_recv):
    rows, cols, slabs = sizes
    height, width, depth, _ = f_hbm.shape
    part = height // CHUNKS
    me_row, me_col, me_slab = (lax.axis_index(axis) for axis in ("rows", "cols", "slabs"))
    partner = {"rows": 1 - me_row}
    peers = (
        {"cols": lax.rem(me_col + cols - 1, cols)},
        {"cols": lax.rem(me_col + 1, cols)},
        {"slabs": lax.rem(me_slab + slabs - 1, slabs)},
        {"slabs": lax.rem(me_slab + 1, slabs)},
    )
    inner_x, inner_z = pl.ds(1, width), pl.ds(Z, depth)

    def load(chunk):
        return pltpu.make_async_copy(
            f_hbm.at[pl.ds(chunk * part, part)],
            field.at[0, pl.ds(1 + chunk * part, part), inner_x, inner_z],
            send_sem.at[chunk],
        )

    load_crowd = pltpu.make_async_copy(c_hbm, crowd, stat_send)

    def face(slot, chunk, side):
        part_rows = pl.ds(1 + chunk * part, part)
        source, target = (
            ((1, inner_z), (width + 1, inner_z)),
            ((width, inner_z), (0, inner_z)),
            ((inner_x, Z), (inner_x, Z + depth)),
            ((inner_x, Z + depth - 1), (inner_x, Z - 1)),
        )[side]
        return pltpu.make_async_remote_copy(
            src_ref=field.at[(slot, part_rows) + source],
            dst_ref=field.at[(slot, part_rows) + target],
            send_sem=send_sem.at[chunk],
            recv_sem=recv_sem.at[slot, chunk],
            device_id=peers[side],
            device_id_type=MESH,
        )

    def edge_row(slot, side):
        source, target = ((1, height + 1), (height, 0))[side]
        return pltpu.make_async_remote_copy(
            src_ref=field.at[slot, source, inner_x, inner_z],
            dst_ref=field.at[slot, target, inner_x, inner_z],
            send_sem=row_send.at[side],
            recv_sem=row_recv.at[slot, side],
            device_id=partner,
            device_id_type=MESH,
        )

    def on_edges(chunk, act):
        @pl.when(chunk == 0)
        def _():
            act(0)

        @pl.when(chunk == CHUNKS - 1)
        def _():
            act(1)

    def send(slot, chunk):
        for side in range(4):
            face(slot, chunk, side).start()
        on_edges(chunk, lambda side: edge_row(slot, side).start())

    def wait_faces(sem):
        four_faces = crowd.at[pl.ds(0, part * 2 * (width + depth) // (width * depth))]
        pltpu.make_async_copy(four_faces, four_faces, sem).wait()

    def sent(chunk):
        wait_faces(send_sem.at[chunk])
        on_edges(chunk, lambda side: edge_row(0, side).wait_send())

    def arrived(slot, chunk):
        wait_faces(recv_sem.at[slot, chunk])
        on_edges(chunk, lambda side: edge_row(slot, 1 - side).wait_recv())

    def advance(slot, chunk, store):
        def row(step, _):
            y = chunk * part + step
            centre = [field[slot, y + 1, x, inner_z] for x in range(width + 2)]
            values = []
            for x in range(width):
                value = centre[x + 1]
                around = (
                    (field[slot, y, x + 1, inner_z] + field[slot, y + 2, x + 1, inner_z])
                    + (centre[x] + centre[x + 2])
                    + (field[slot, y + 1, x + 1, pl.ds(Z - 1, depth)] + field[slot, y + 1, x + 1, pl.ds(Z + 1, depth)])
                )
                values.append(0.1 * around + value * (0.6 - (0.2 * value) * crowd[y, x]))
            for x in range(width):
                store(y, x, values[x])
            return 0

        lax.fori_loop(0, part, row, 0)

    barrier = pltpu.get_barrier_semaphore()
    for peer in peers + (partner,):
        pl.semaphore_signal(barrier, inc=1, device_id=peer, device_id_type=MESH)
    for chunk in range(CHUNKS):
        load(chunk).start()
    pl.semaphore_wait(barrier, len(peers) + 1)

    def begin(chunk, _):
        load(chunk).wait()
        send(0, chunk)
        return 0

    lax.fori_loop(0, CHUNKS, begin, 0)
    load_crowd.start()
    load_crowd.wait()

    def one_step(step, _):
        slot = lax.rem(step, 2)
        other = 1 - slot

        def one_chunk(place, _):
            chunk = place
            arrived(slot, chunk)

            def store(y, x, value):
                field[other, y + 1, x + 1, inner_z] = value

            advance(slot, chunk, store)
            sent(chunk)
            send(other, chunk)
            return 0

        lax.fori_loop(0, CHUNKS, one_chunk, 0)
        return 0

    lax.fori_loop(0, STEPS - 1, one_step, 0)

    step = STEPS - 1
    slot = step % 2

    def last_chunk(place, _):
        chunk = place
        arrived(slot, chunk)

        def store(y, x, value):
            end_ref[y, x] = value

        advance(slot, chunk, store)

        @pl.when(place == 0)
        def _():
            for x in range(width):
                shift[x] = end_ref[chunk * part, x]
                first[x] = jnp.zeros_like(first[x])
                second[x] = jnp.zeros_like(second[x])

        for x in range(width):
            middle = shift[x]
            one, two = first[x], second[x]
            for y in range(part):
                moved = end_ref[chunk * part + y, x] - middle
                one, two = one + moved, two + moved * moved
            first[x], second[x] = one, two
        return 0

    lax.fori_loop(0, CHUNKS, last_chunk, 0)

    for x in range(width):
        mine[0, x] = shift[x] + first[x] * (1.0 / height)
        mine[1, x] = second[x] - first[x] * first[x] * (1.0 / height)
    swap = pltpu.make_async_remote_copy(
        src_ref=mine,
        dst_ref=theirs,
        send_sem=stat_send,
        recv_sem=stat_recv,
        device_id=partner,
        device_id_type=MESH,
    )
    swap.start()

    def drain(chunk, _):
        sent(chunk)
        return 0

    lax.fori_loop(0, CHUNKS, drain, 0)
    swap.wait()


def finish(end_ref, mine, theirs, standardized_hbm, end_hbm, standardized, mean_ref, scale_ref, out_sem, end_sem):
    height, width = end_ref.shape[:2]
    part = height // CHUNKS

    copy_end = pltpu.make_async_copy(end_ref, end_hbm, end_sem)

    def copy_out(chunk):
        part_rows = pl.ds(chunk * part, part)
        return pltpu.make_async_copy(standardized.at[part_rows], standardized_hbm.at[part_rows], out_sem)

    copy_end.start()
    for x in range(width):
        apart = mine[0, x] - theirs[0, x]
        total = mine[1, x] + theirs[1, x] + apart * apart * (0.5 * height)
        mean_ref[x] = 0.5 * (mine[0, x] + theirs[0, x])
        scale_ref[x] = lax.rsqrt(total * (0.5 / height) + 0.0001)
    for chunk in range(CHUNKS):

        def row(step, _):
            y = chunk * part + step
            for x in range(width):
                standardized[y, x] = (end_ref[y, x] - mean_ref[x]) * scale_ref[x]
            return 0

        lax.fori_loop(0, part, row, 0)
        copy_out(chunk).start()
    pltpu.make_async_copy(standardized, standardized_hbm, out_sem).wait()
    copy_end.wait()


def local(sizes, field_values, crowding):
    height, width, depth, lanes = field_values.shape
    whole = jax.ShapeDtypeStruct(field_values.shape, jnp.float32)
    pair = jax.ShapeDtypeStruct((2, width, depth, lanes), jnp.float32)
    vmem, anywhere = pl.BlockSpec(memory_space=pltpu.VMEM), pl.BlockSpec(memory_space=pl.ANY)
    plane = pltpu.VMEM((width, depth, lanes), jnp.float32)
    end, mine, theirs = pl.pallas_call(
        functools.partial(evolve, sizes),
        out_shape=tuple(pltpu.VMEM(kind.shape, jnp.float32) for kind in (whole, pair, pair)),
        in_specs=[anywhere, anywhere],
        out_specs=(vmem, vmem, vmem),
        scratch_shapes=[
            pltpu.VMEM((2, height + 2, width + 2, 3 * depth, lanes), jnp.float32),
            pltpu.VMEM((height, width, depth, lanes), jnp.float32),
            plane,
            plane,
            plane,
            pltpu.SemaphoreType.DMA((CHUNKS,)),
            pltpu.SemaphoreType.DMA((2, CHUNKS)),
            pltpu.SemaphoreType.DMA((2,)),
            pltpu.SemaphoreType.DMA((2, 2)),
            pltpu.SemaphoreType.DMA,
            pltpu.SemaphoreType.DMA,
        ],
        compiler_params=pltpu.CompilerParams(collective_id=0, has_side_effects=True),
        name="evolve",
    )(field_values, crowding)
    return pl.pallas_call(
        finish,
        out_shape=(whole, whole),
        in_specs=[vmem, vmem, vmem],
        out_specs=(anywhere, anywhere),
        scratch_shapes=[
            pltpu.VMEM((height, width, depth, lanes), jnp.float32),
            plane,
            plane,
            pltpu.SemaphoreType.DMA,
            pltpu.SemaphoreType.DMA,
        ],
        name="finish",
    )(*(pltpu.with_memory_space_constraint(value, pltpu.VMEM) for value in (end, mine, theirs)))


def solution(mesh):
    spec = P(("site", "rows"), "cols", "slabs", None)
    sizes = tuple(mesh.shape[axis] for axis in ("rows", "cols", "slabs"))
    return jax.shard_map(
        functools.partial(local, sizes),
        mesh=mesh,
        in_specs=(spec, spec),
        out_specs=(spec, spec),
        check_vma=False,
    )
```
